8 devices in a mesh: ep: 4 (over z, y, x), dp: 2 (over core).
Axes of the slice: x: 2, y: 2, z: 1, core: 2. Of those that a mesh axis runs over, the one named last changes fastest.
Arguments:
- tokens: bfloat16 [4096, 768], P(('dp', 'ep'))
- d_out: bfloat16 [4096, 768], P(('dp', 'ep'))
- expert_ids: int32 [2, 4096, 4], P(None, ('dp', 'ep'))
- gate_vals: float32 [2, 4096, 4], P(None, ('dp', 'ep'))
- w_mix: bfloat16 [2, 768, 768], replicated
- w_gate: bfloat16 [2, 16, 768, 1344], P(None, 'ep')
- w_up: bfloat16 [2, 16, 768, 1344], P(None, 'ep')
- w_down: bfloat16 [2, 16, 1344, 768], P(None, 'ep')
Outputs:
- output 1: bfloat16 [4096, 768], P(('dp', 'ep'))
- output 2: bfloat16 [4096, 768], P(('dp', 'ep'))
- output 3: bfloat16 [2, 768, 768], replicated
- output 4: bfloat16 [2, 16, 768, 1344], P(None, 'ep')
- output 5: bfloat16 [2, 16, 768, 1344], P(None, 'ep')
- output 6: bfloat16 [2, 16, 1344, 768], P(None, 'ep')
All inputs are finite; a program needn't handle non-finite values.
Results may differ from the reference program's by a relative error of at most 0.0179635.
Values are sent between devices in bfloat16 or wider.
A program may use at most 1 GiB of HBM per device.

```python
import jax
import jax.numpy as jnp

D = 768
FF = 1344
EXPERTS = 16
TOP = 4
TOK = 512
NDEV = 8
LAYERS = 2
CAP = 384
HOT = 2

N_TOK = TOK * NDEV
CAP_ALL = CAP * NDEV


def route_device(hot_mask, dev_key):
    key_rest, key_run, key_tok = jax.random.split(dev_key, 3)
    rest_copies = TOK * TOP - HOT * CAP
    base_count = rest_copies // (EXPERTS - HOT)
    extra_count = rest_copies % (EXPERTS - HOT)
    shuffled = jax.random.permutation(key_rest, EXPERTS)
    cold_sorted = 1 - hot_mask[shuffled]
    cold_rank = jnp.cumsum(cold_sorted) - 1
    bonus_sorted = cold_sorted * (cold_rank < extra_count).astype(jnp.int32)
    bonus = jnp.zeros((EXPERTS,), jnp.int32).at[shuffled].set(bonus_sorted)
    counts = jnp.where(hot_mask == 1, CAP, base_count + bonus)
    run_order = jax.random.permutation(key_run, EXPERTS)
    flat_ids = jnp.repeat(run_order, counts[run_order], total_repeat_length=TOK * TOP)
    table = flat_ids.reshape(TOP, TOK).T
    return table[jax.random.permutation(key_tok, TOK)]


def route_layer(layer_key):
    key_hot, key_dev = jax.random.split(layer_key)
    hot_ids = jax.random.permutation(key_hot, EXPERTS)[:HOT]
    hot_mask = jnp.zeros((EXPERTS,), jnp.int32).at[hot_ids].set(1)
    per_device = jax.vmap(route_device, in_axes=(None, 0))(hot_mask, jax.random.split(key_dev, NDEV))
    return per_device.reshape(N_TOK, TOP)


def setup_inputs(seed: int = 0) -> dict:
    keys = jax.random.split(jax.random.key(seed), 8)
    tokens = jax.random.normal(keys[0], (N_TOK, D), jnp.float32).astype(jnp.bfloat16)
    d_out = jax.random.normal(keys[1], (N_TOK, D), jnp.float32).astype(jnp.bfloat16)
    expert_ids = jax.vmap(route_layer)(jax.random.split(keys[2], LAYERS))
    gate_vals = jax.random.uniform(keys[3], (LAYERS, N_TOK, TOP), jnp.float32, 0.5, 1.5) * TOP ** -0.5
    w_mix = (jax.random.normal(keys[4], (LAYERS, D, D), jnp.float32) * D ** -0.5).astype(jnp.bfloat16)
    w_gate = (jax.random.normal(keys[5], (LAYERS, EXPERTS, D, FF), jnp.float32) * D ** -0.5).astype(jnp.bfloat16)
    w_up = (jax.random.normal(keys[6], (LAYERS, EXPERTS, D, FF), jnp.float32) * D ** -0.5).astype(jnp.bfloat16)
    w_down = (jax.random.normal(keys[7], (LAYERS, EXPERTS, FF, D), jnp.float32) * FF ** -0.5).astype(jnp.bfloat16)
    return {'tokens': tokens, 'd_out': d_out, 'expert_ids': expert_ids, 'gate_vals': gate_vals,
            'w_mix': w_mix, 'w_gate': w_gate, 'w_up': w_up, 'w_down': w_down}


def silu_parts(pre_gate):
    sig_val = jax.nn.sigmoid(pre_gate)
    return pre_gate * sig_val, sig_val * (1.0 + pre_gate * (1.0 - sig_val))


def copy_slots(expert_ids):
    flat_ids = expert_ids.reshape(-1)
    sort_order = jnp.argsort(flat_ids, stable=True)
    sorted_ids = flat_ids[sort_order]
    counts = jnp.bincount(flat_ids, length=EXPERTS)
    starts = jnp.cumsum(counts) - counts
    rows_sorted = sorted_ids * CAP_ALL + jnp.arange(flat_ids.shape[0]) - starts[sorted_ids]
    return jnp.zeros_like(flat_ids).at[sort_order].set(rows_sorted)


def layer_forward(x_in, expert_ids, gate_vals, w_mix, w_gate, w_up, w_down):
    mixed = x_in.astype(jnp.float32) + jnp.dot(x_in, w_mix, preferred_element_type=jnp.float32)
    u_act = mixed.astype(jnp.bfloat16)
    copy_rows = copy_slots(expert_ids)
    copy_tok = jnp.arange(N_TOK * TOP) // TOP
    expert_in = jnp.zeros((EXPERTS * CAP_ALL, D), jnp.bfloat16).at[copy_rows].set(u_act[copy_tok])
    expert_in = expert_in.reshape(EXPERTS, CAP_ALL, D)
    expert_f = expert_in.astype(jnp.float32)
    pre_gate = jnp.einsum('ecd,edf->ecf', expert_f, w_gate.astype(jnp.float32))
    pre_up = jnp.einsum('ecd,edf->ecf', expert_f, w_up.astype(jnp.float32))
    act, _ = silu_parts(pre_gate)
    hidden = (act * pre_up).astype(jnp.bfloat16)
    expert_out = jnp.einsum('ecf,efd->ecd', hidden.astype(jnp.float32), w_down.astype(jnp.float32)).astype(jnp.bfloat16)
    out_copy = expert_out.reshape(EXPERTS * CAP_ALL, D)[copy_rows].reshape(N_TOK, TOP, D)
    y_out = u_act.astype(jnp.float32) + jnp.sum(gate_vals[:, :, None] * out_copy.astype(jnp.float32), axis=1)
    return y_out.astype(jnp.bfloat16), (x_in, copy_rows, expert_in, pre_gate, pre_up, hidden)


def layer_backward(saved, d_y, gate_vals, w_mix, w_gate, w_up, w_down):
    x_in, copy_rows, expert_in, pre_gate, pre_up, hidden = saved
    g_dy = (gate_vals[:, :, None] * d_y.astype(jnp.float32)[:, None, :]).astype(jnp.bfloat16).reshape(N_TOK * TOP, D)
    d_buf = jnp.zeros((EXPERTS * CAP_ALL, D), jnp.bfloat16).at[copy_rows].set(g_dy).reshape(EXPERTS, CAP_ALL, D)
    d_buf_f = d_buf.astype(jnp.float32)
    d_hidden = jnp.einsum('ecd,efd->ecf', d_buf_f, w_down.astype(jnp.float32))
    act, act_slope = silu_parts(pre_gate)
    d_pre_gate = (d_hidden * pre_up * act_slope).astype(jnp.bfloat16).astype(jnp.float32)
    d_pre_up = (d_hidden * act).astype(jnp.bfloat16).astype(jnp.float32)
    d_expert_in = (jnp.einsum('ecf,edf->ecd', d_pre_gate, w_gate.astype(jnp.float32))
                   + jnp.einsum('ecf,edf->ecd', d_pre_up, w_up.astype(jnp.float32))).astype(jnp.bfloat16)
    expert_f = expert_in.astype(jnp.float32)
    g_gate = jnp.einsum('ecd,ecf->edf', expert_f, d_pre_gate).astype(jnp.bfloat16)
    g_up = jnp.einsum('ecd,ecf->edf', expert_f, d_pre_up).astype(jnp.bfloat16)
    g_down = jnp.einsum('ecf,ecd->efd', hidden.astype(jnp.float32), d_buf_f).astype(jnp.bfloat16)
    d_copy = d_expert_in.reshape(EXPERTS * CAP_ALL, D)[copy_rows].reshape(N_TOK, TOP, D)
    d_u = (d_y.astype(jnp.float32) + jnp.sum(gate_vals[:, :, None] * d_copy.astype(jnp.float32), axis=1)).astype(jnp.bfloat16)
    g_mix = jnp.dot(x_in.T, d_u, preferred_element_type=jnp.float32).astype(jnp.bfloat16)
    d_x = (d_u.astype(jnp.float32) + jnp.dot(d_u, w_mix.T, preferred_element_type=jnp.float32)).astype(jnp.bfloat16)
    return d_x, (g_mix, g_gate, g_up, g_down)


def reference(tokens, d_out, expert_ids, gate_vals, w_mix, w_gate, w_up, w_down):
    layer_in = tokens
    saved_all = []
    for layer in range(LAYERS):
        layer_in, saved = layer_forward(layer_in, expert_ids[layer], gate_vals[layer], w_mix[layer],
                                        w_gate[layer], w_up[layer], w_down[layer])
        saved_all.append(saved)
    d_y = d_out
    grads = []
    for layer in reversed(range(LAYERS)):
        d_y, grad_set = layer_backward(saved_all[layer], d_y, gate_vals[layer], w_mix[layer],
                                       w_gate[layer], w_up[layer], w_down[layer])
        grads.insert(0, grad_set)
    return (layer_in, d_y,
            jnp.stack([entry[0] for entry in grads]),
            jnp.stack([entry[1] for entry in grads]),
            jnp.stack([entry[2] for entry in grads]),
            jnp.stack([entry[3] for entry in grads]))
```

```python
import functools

import jax
import jax.numpy as jnp
from jax import lax
from jax.experimental import pallas as pl
from jax.experimental.pallas import tpu as pltpu
from jax.sharding import PartitionSpec as P

TILE = 384
SUB = 128
ALIGN = 16
F_CHUNK = 512
VMEM_LIMIT = 66 * 1024 * 1024 - 4 * 1024 * 1024


def silu_parts(pre_gate):
    sig_val = jax.nn.sigmoid(pre_gate)
    return pre_gate * sig_val, sig_val * (1.0 + pre_gate * (1.0 - sig_val))


def dot_nn(lhs, rhs):
    return lax.dot_general(lhs, rhs, (((1,), (0,)), ((), ())), preferred_element_type=jnp.float32)


def dot_nt(lhs, rhs):
    return lax.dot_general(lhs, rhs, (((1,), (1,)), ((), ())), preferred_element_type=jnp.float32)


def dot_tn(lhs, rhs):
    return lax.dot_general(lhs, rhs, (((0,), (0,)), ((), ())), preferred_element_type=jnp.float32)


def f_chunks(width):
    return [(lo, min(F_CHUNK, width - lo)) for lo in range(0, width, F_CHUNK)]


def row_offsets(count_ref, expert, n_src):
    counts = [count_ref[expert, src] for src in range(n_src)]
    offsets = [jnp.int32(0)]
    for count in counts:
        offsets.append(offsets[-1] + (count + ALIGN - 1) // ALIGN * ALIGN)
    total = offsets.pop()
    return counts, offsets, jnp.maximum((total + TILE - 1) // TILE, 1)


def sub_hot(rank_ref, src, block, dtype):
    tok = rank_ref.shape[2]
    want = lax.broadcasted_iota(jnp.int32, (SUB, tok), 0) + block * SUB
    return (rank_ref[0, src:src + 1, :] == want).astype(dtype)


def combine(counts, offsets, rank_t_ref, gate_t_ref, buf, acc):
    tok = rank_t_ref.shape[1]
    cap = (tok * 3 // 4 + SUB - 1) // SUB * SUB

    def add(src, width):
        want = lax.broadcasted_iota(jnp.int32, (tok, width), 1)
        pick = (rank_t_ref[0, :, src:src + 1] == want).astype(jnp.bfloat16)
        rows = buf[pl.ds(pl.multiple_of(offsets[src], ALIGN), width), :]
        acc[src] += gate_t_ref[0, :, src:src + 1] * dot_nn(pick, rows)

    for src in range(len(counts)):
        pl.when(jnp.logical_and(counts[src] > 0, counts[src] <= SUB))(functools.partial(add, src, SUB))
        pl.when(counts[src] > SUB)(functools.partial(add, src, cap))


def forward_kernel(count_ref, u_ref, rank_ref, rank_t_ref, gate_t_ref, wg_ref, wu_ref, wd_ref, out_ref,
                   x_buf, o_buf, h_buf, acc):
    expert = pl.program_id(0)
    n_src = u_ref.shape[0]

    @pl.when(expert == 0)
    def _():
        acc[...] = jnp.zeros_like(acc)
        o_buf[...] = jnp.zeros_like(o_buf)

    counts, offsets, tiles = row_offsets(count_ref, expert, n_src)
    x_buf[pl.ds(pl.multiple_of((tiles - 1) * TILE, TILE), TILE), :] = jnp.zeros((TILE, x_buf.shape[1]), x_buf.dtype)
    for src in range(n_src):
        def gather(block, carry, src=src):
            rows = dot_nn(sub_hot(rank_ref, src, block, jnp.bfloat16), u_ref[src])
            x_buf[pl.ds(pl.multiple_of(offsets[src] + block * SUB, ALIGN), SUB), :] = rows.astype(jnp.bfloat16)
            return carry
        lax.fori_loop(0, (counts[src] + SUB - 1) // SUB, gather, 0)

    def tile_step(tile, carry):
        span = pl.ds(pl.multiple_of(tile * TILE, TILE), TILE)
        rows = x_buf[span, :]
        for lo, width in f_chunks(wg_ref.shape[2]):
            cols = slice(lo, lo + width)
            pre_gate = dot_nt(rows, wg_ref[0, 0, cols, :])
            pre_up = dot_nt(rows, wu_ref[0, 0, cols, :])
            act, _ = silu_parts(pre_gate)
            h_buf[:, cols] = (act * pre_up).astype(jnp.bfloat16)
        o_buf[span, :] = dot_nn(h_buf[...], wd_ref[0, 0]).astype(jnp.bfloat16)
        return carry
    lax.fori_loop(0, tiles, tile_step, 0)

    combine(counts, offsets, rank_t_ref, gate_t_ref, o_buf, acc)

    @pl.when(expert == pl.num_programs(0) - 1)
    def _():
        out_ref[...] = acc[...].astype(jnp.bfloat16)


def backward_kernel(count_ref, u_ref, dy_ref, rank_ref, gate_ref, rank_t_ref, gate_t_ref, wg_ref, wu_ref, wd_ref,
                    out_ref, dg_out, du_out, dw_out,
                    x_buf, c_buf, h_buf, da_buf, db_buf, acc, dg_acc, du_acc, dw_acc, dg_st, du_st, dw_st, sems):
    expert = pl.program_id(0)
    last = pl.num_programs(0) - 1
    n_src = u_ref.shape[0]

    @pl.when(expert == 0)
    def _():
        acc[...] = jnp.zeros_like(acc)
        x_buf[...] = jnp.zeros_like(x_buf)

    counts, offsets, tiles = row_offsets(count_ref, expert, n_src)
    tail = pl.ds(pl.multiple_of((tiles - 1) * TILE, TILE), TILE)
    x_buf[tail, :] = jnp.zeros((TILE, x_buf.shape[1]), x_buf.dtype)
    c_buf[tail, :] = jnp.zeros((TILE, c_buf.shape[1]), c_buf.dtype)
    for src in range(n_src):
        def gather(block, carry, src=src):
            hot = sub_hot(rank_ref, src, block, jnp.float32)
            pick = hot.astype(jnp.bfloat16)
            span = pl.ds(pl.multiple_of(offsets[src] + block * SUB, ALIGN), SUB)
            gate = jnp.sum(hot * gate_ref[0, src:src + 1, :], axis=1, keepdims=True)
            x_buf[span, :] = dot_nn(pick, u_ref[src]).astype(jnp.bfloat16)
            c_buf[span, :] = (gate * dot_nn(pick, dy_ref[src])).astype(jnp.bfloat16)
            return carry
        lax.fori_loop(0, (counts[src] + SUB - 1) // SUB, gather, 0)

    def tile_step(tile, carry):
        first = tile == 0
        span = pl.ds(pl.multiple_of(tile * TILE, TILE), TILE)
        rows = x_buf[span, :]
        grads = c_buf[span, :]
        for lo, width in f_chunks(wg_ref.shape[2]):
            cols = slice(lo, lo + width)
            pre_gate = dot_nt(rows, wg_ref[0, 0, cols, :])
            pre_up = dot_nt(rows, wu_ref[0, 0, cols, :])
            d_hid = dot_nt(grads, wd_ref[0, 0, cols, :])
            act, slope = silu_parts(pre_gate)
            h_buf[:, cols] = (act * pre_up).astype(jnp.bfloat16)
            da_buf[:, cols] = (d_hid * pre_up * slope).astype(jnp.bfloat16)
            db_buf[:, cols] = (d_hid * act).astype(jnp.bfloat16)
        x_buf[span, :] = (dot_nn(da_buf[...], wg_ref[0, 0]) + dot_nn(db_buf[...], wu_ref[0, 0])).astype(jnp.bfloat16)
        for lo, width in f_chunks(wg_ref.shape[2]):
            cols = slice(lo, lo + width)
            dg_acc[cols, :] = jnp.where(first, 0.0, dg_acc[cols, :]) + dot_tn(da_buf[:, cols], rows)
            du_acc[cols, :] = jnp.where(first, 0.0, du_acc[cols, :]) + dot_tn(db_buf[:, cols], rows)
            dw_acc[cols, :] = jnp.where(first, 0.0, dw_acc[cols, :]) + dot_tn(h_buf[:, cols], grads)
        return carry
    lax.fori_loop(0, tiles, tile_step, 0)

    combine(counts, offsets, rank_t_ref, gate_t_ref, x_buf, acc)

    def copies(index):
        return [pltpu.make_async_copy(src, dst.at[index], sems.at[i])
                for i, (src, dst) in enumerate(((dg_st, dg_out), (du_st, du_out), (dw_st, dw_out)))]

    @pl.when(expert > 0)
    def _():
        for copy in copies(expert - 1):
            copy.wait()

    dg_st[...] = dg_acc[...].astype(jnp.bfloat16)
    du_st[...] = du_acc[...].astype(jnp.bfloat16)
    dw_st[...] = dw_acc[...].astype(jnp.bfloat16)
    for copy in copies(expert):
        copy.start()

    @pl.when(expert == last)
    def _():
        out_ref[...] = acc[...].astype(jnp.bfloat16)
        for copy in copies(expert):
            copy.wait()


def whole_vmem():
    return pl.BlockSpec(memory_space=pltpu.VMEM)


def per_expert(shape):
    rest = (0,) * (len(shape) - 1)
    return pl.BlockSpec((1,) + tuple(shape[1:]), lambda e, *_: (e,) + rest)


def layer_weight(layer, shape):
    return pl.BlockSpec((1, 1) + tuple(shape[2:]), lambda e, *_: (layer, e, 0, 0))


def expert_forward(layer, u_all, tables, w_gate, w_up, w_down):
    n_src, tok, d_model = u_all.shape
    _, n_local, width, _ = w_gate.shape
    counts, rank, gate, rank_t, gate_t = tables
    rows_max = n_src * (tok * 3 // 4) + SUB
    rows_max = (rows_max + TILE - 1) // TILE * TILE
    flops = 3 * 2 * (n_src * tok) * d_model * width * 3 // 2
    return pl.pallas_call(
        forward_kernel,
        out_shape=jax.ShapeDtypeStruct((n_src, tok, d_model), jnp.bfloat16),
        grid_spec=pltpu.PrefetchScalarGridSpec(
            num_scalar_prefetch=1,
            grid=(n_local,),
            in_specs=[whole_vmem(), per_expert(rank.shape), per_expert(rank_t.shape), per_expert(gate_t.shape),
                      layer_weight(layer, w_gate.shape), layer_weight(layer, w_up.shape),
                      layer_weight(layer, w_down.shape)],
            out_specs=whole_vmem(),
            scratch_shapes=[pltpu.VMEM((rows_max, d_model), jnp.bfloat16),
                            pltpu.VMEM((rows_max, d_model), jnp.bfloat16),
                            pltpu.VMEM((TILE, width), jnp.bfloat16),
                            pltpu.VMEM((n_src, tok, d_model), jnp.float32)]),
        compiler_params=pltpu.CompilerParams(vmem_limit_bytes=VMEM_LIMIT),
        cost_estimate=pl.CostEstimate(flops=flops, bytes_accessed=3 * 2 * n_local * d_model * width, transcendentals=0),
        name='expert_forward',
    )(counts, u_all, rank, rank_t, gate_t, w_gate, w_up, w_down)


def expert_backward(layer, u_all, dy_all, tables, w_gate, w_up, w_down):
    n_src, tok, d_model = u_all.shape
    _, n_local, width, _ = w_gate.shape
    counts, rank, gate, rank_t, gate_t = tables
    rows_max = n_src * (tok * 3 // 4) + SUB
    rows_max = (rows_max + TILE - 1) // TILE * TILE
    flops = 8 * 2 * (n_src * tok) * d_model * width * 3 // 2
    any_spec = pl.BlockSpec(memory_space=pl.ANY)
    return pl.pallas_call(
        backward_kernel,
        out_shape=(jax.ShapeDtypeStruct((n_src, tok, d_model), jnp.bfloat16),
                   jax.ShapeDtypeStruct(w_gate.shape[1:], jnp.bfloat16),
                   jax.ShapeDtypeStruct(w_up.shape[1:], jnp.bfloat16),
                   jax.ShapeDtypeStruct(w_down.shape[1:], jnp.bfloat16)),
        grid_spec=pltpu.PrefetchScalarGridSpec(
            num_scalar_prefetch=1,
            grid=(n_local,),
            in_specs=[whole_vmem(), whole_vmem(), per_expert(rank.shape), per_expert(gate.shape),
                      per_expert(rank_t.shape), per_expert(gate_t.shape),
                      layer_weight(layer, w_gate.shape), layer_weight(layer, w_up.shape),
                      layer_weight(layer, w_down.shape)],
            out_specs=(whole_vmem(), any_spec, any_spec, any_spec),
            scratch_shapes=[pltpu.VMEM((rows_max, d_model), jnp.bfloat16),
                            pltpu.VMEM((rows_max, d_model), jnp.bfloat16),
                            pltpu.VMEM((TILE, width), jnp.bfloat16),
                            pltpu.VMEM((TILE, width), jnp.bfloat16),
                            pltpu.VMEM((TILE, width), jnp.bfloat16),
                            pltpu.VMEM((n_src, tok, d_model), jnp.float32),
                            pltpu.VMEM((width, d_model), jnp.float32),
                            pltpu.VMEM((width, d_model), jnp.float32),
                            pltpu.VMEM((width, d_model), jnp.float32),
                            pltpu.VMEM((width, d_model), jnp.bfloat16),
                            pltpu.VMEM((width, d_model), jnp.bfloat16),
                            pltpu.VMEM((width, d_model), jnp.bfloat16),
                            pltpu.SemaphoreType.DMA((3,))]),
        compiler_params=pltpu.CompilerParams(vmem_limit_bytes=VMEM_LIMIT),
        cost_estimate=pl.CostEstimate(flops=flops, bytes_accessed=6 * 2 * n_local * d_model * width, transcendentals=0),
        name='expert_backward',
    )(counts, u_all, dy_all, rank, gate, rank_t, gate_t, w_gate, w_up, w_down)


def route_tables(expert_ids, gate_vals, n_local):
    packed = jnp.concatenate([expert_ids.astype(jnp.float32), gate_vals], axis=2)
    packed = lax.all_gather(packed, 'ep')
    top_k = expert_ids.shape[2]
    tok = expert_ids.shape[1]
    ids = packed[..., :top_k].astype(jnp.int32)
    gates = packed[..., top_k:]
    mine = lax.axis_index('ep') * n_local + jnp.arange(n_local)
    hits = ids[:, :, None] == mine[None, None, :, None, None]
    chosen = jnp.any(hits, axis=-1)
    gate = jnp.sum(jnp.where(hits, gates[:, :, None], 0.0), axis=-1)
    upto = (jnp.arange(tok)[:, None] <= jnp.arange(tok)[None, :]).astype(jnp.bfloat16)
    order = jnp.einsum('slet,tv->slev', chosen.astype(jnp.bfloat16), upto, preferred_element_type=jnp.float32)
    counts = order[..., -1].astype(jnp.int32)
    rank = jnp.where(chosen, order.astype(jnp.int32) - 1, -1)
    return [(counts[:, layer].T, rank[:, layer].transpose(1, 0, 2), gate[:, layer].transpose(1, 0, 2),
             rank[:, layer].transpose(1, 2, 0), gate[:, layer].transpose(1, 2, 0))
            for layer in range(expert_ids.shape[0])]


def token_sum(own, parts):
    parts = lax.all_to_all(parts, 'ep', 0, 0, tiled=True)
    return (own.astype(jnp.float32) + jnp.sum(parts.astype(jnp.float32), axis=0)).astype(jnp.bfloat16)


def stack_part(grads, index):
    return jnp.stack([entry[index] for entry in grads])


def solution(mesh):
    tok_spec = P(('dp', 'ep'), None)
    route_spec = P(None, ('dp', 'ep'), None)
    whole_spec = P(None, None, None)
    expert_spec = P(None, 'ep', None, None)

    def device_step(tokens, d_out, expert_ids, gate_vals, w_mix, w_gate, w_up, w_down):
        n_layers = w_mix.shape[0]
        tables = route_tables(expert_ids, gate_vals, w_gate.shape[1])
        w_gate_t = jnp.swapaxes(w_gate, 2, 3)
        w_up_t = jnp.swapaxes(w_up, 2, 3)
        layer_in = tokens
        saved = []
        for layer in range(n_layers):
            mixed = layer_in.astype(jnp.float32) + jnp.dot(layer_in, w_mix[layer], preferred_element_type=jnp.float32)
            u_act = mixed.astype(jnp.bfloat16)
            u_all = lax.all_gather(u_act, 'ep')
            parts = expert_forward(layer, u_all, tables[layer], w_gate_t, w_up_t, w_down)
            saved.append((layer_in, u_all))
            layer_in = token_sum(u_act, parts)
        d_y = d_out
        grads = []
        for layer in reversed(range(n_layers)):
            x_in, u_all = saved[layer]
            dy_all = lax.all_gather(d_y, 'ep')
            parts, g_gate, g_up, g_down = expert_backward(layer, u_all, dy_all, tables[layer],
                                                          w_gate_t, w_up_t, w_down)
            g_gate = lax.psum(g_gate, 'dp')
            g_up = lax.psum(g_up, 'dp')
            g_down = lax.psum(g_down, 'dp')
            d_u = token_sum(d_y, parts)
            g_mix = jnp.einsum('td,te->de', x_in, d_u, preferred_element_type=jnp.float32).astype(jnp.bfloat16)
            g_mix = lax.psum(g_mix, ('dp', 'ep'))
            d_y = (d_u.astype(jnp.float32)
                   + jnp.einsum('te,de->td', d_u, w_mix[layer], preferred_element_type=jnp.float32)).astype(jnp.bfloat16)
            grads.insert(0, (g_mix, g_gate, g_up, g_down))
        return (layer_in, d_y, stack_part(grads, 0), jnp.swapaxes(stack_part(grads, 1), 2, 3),
                jnp.swapaxes(stack_part(grads, 2), 2, 3), stack_part(grads, 3))

    return jax.shard_map(device_step, mesh=mesh,
                         in_specs=(tok_spec, tok_spec, route_spec, route_spec, whole_spec,
                                   expert_spec, expert_spec, expert_spec),
                         out_specs=(tok_spec, tok_spec, whole_spec, expert_spec, expert_spec, expert_spec),
                         check_vma=False)
```

```python
import functools

import jax
import jax.numpy as jnp
from jax import lax
from jax.experimental import pallas as pl
from jax.experimental.pallas import tpu as pltpu
from jax.sharding import PartitionSpec as P


TILE = 384
SUB = 128
ALIGN = 16
F_CHUNK = 512
SOURCES = 4
VMEM_LIMIT = 62 * 1024 * 1024
BF16 = jnp.bfloat16
F32 = jnp.float32


def silu_parts(pre_gate):
    sig_val = jax.nn.sigmoid(pre_gate)
    return pre_gate * sig_val, sig_val * (1.0 + pre_gate * (1.0 - sig_val))


def dot_nn(lhs, rhs):
    return lax.dot_general(lhs, rhs, (((1,), (0,)), ((), ())), preferred_element_type=F32)


def dot_nt(lhs, rhs):
    return lax.dot_general(lhs, rhs, (((1,), (1,)), ((), ())), preferred_element_type=F32)


def dot_tn(lhs, rhs):
    return lax.dot_general(lhs, rhs, (((0,), (0,)), ((), ())), preferred_element_type=F32)


def f_chunks(width):
    return [slice(lo, min(lo + F_CHUNK, width)) for lo in range(0, width, F_CHUNK)]


def tile_span(tile):
    return pl.ds(pl.multiple_of(tile * TILE, TILE), TILE)


def row_offsets(count_ref, expert):
    counts = [count_ref[expert, src] for src in range(SOURCES)]
    offsets = [jnp.int32(0)]
    for count in counts:
        offsets.append(offsets[-1] + (count + ALIGN - 1) // ALIGN * ALIGN)
    total = offsets.pop()
    return counts, offsets, jnp.maximum((total + TILE - 1) // TILE, 1)


def per_source(counts, run, capacity):
    small = functools.reduce(jnp.maximum, counts) <= SUB

    @pl.when(small)
    def _():
        for src in range(SOURCES):
            run(src, SUB)

    @pl.when(jnp.logical_not(small))
    def _():
        for src in range(SOURCES):
            pl.when(counts[src] <= SUB)(functools.partial(run, src, SUB))
            pl.when(counts[src] > SUB)(functools.partial(run, src, capacity))


def fetch(pieces, buf, sems, base):
    copies, row = [], 0
    for index, piece in enumerate(pieces):
        rows = piece.shape[0]
        copies.append(pltpu.make_async_copy(piece, buf.at[pl.ds(row, rows)], sems.at[base + index]))
        row += rows
    return copies


def gather(counts, offsets, rank_ref, capacity, tok, write):
    def run(src, rows):
        want = lax.broadcasted_iota(jnp.int32, (rows, tok), 0)
        hot = (rank_ref[0, src:src + 1, :] == want).astype(F32)
        write(src, hot, pl.ds(pl.multiple_of(offsets[src], ALIGN), rows))

    per_source(counts, run, capacity)


def combine(counts, offsets, rank_t_ref, gate_t_ref, buf, acc, capacity, tok):
    def run(src, rows):
        want = lax.broadcasted_iota(jnp.int32, (tok, rows), 1)
        pick = (rank_t_ref[0, :, src:src + 1] == want).astype(BF16)
        values = buf[pl.ds(pl.multiple_of(offsets[src], ALIGN), rows), :]
        span = slice(src * tok, (src + 1) * tok)
        acc[span, :] += gate_t_ref[0, :, src:src + 1] * dot_nn(pick, values)

    per_source(counts, run, capacity)


def put_out(acc, out_refs):
    row = 0
    for out in out_refs:
        rows = out.shape[0]
        out[...] = acc[row:row + rows, :].astype(BF16)
        row += rows


def forward_kernel(n_in, n_out, capacity, *refs):
    count_ref, refs = refs[0], refs[1:]
    u_pieces, refs = refs[:n_in], refs[n_in:]
    rank_ref, rank_t_ref, gate_t_ref, wg_ref, wu_ref, wd_ref = refs[:6]
    outs, refs = refs[6:6 + n_out], refs[6 + n_out:]
    u_buf, x_buf, o_buf, h_buf, acc, sems = refs
    expert = pl.program_id(0)
    tok = rank_t_ref.shape[1]

    @pl.when(expert == 0)
    def _():
        copies = fetch(u_pieces, u_buf, sems, 0)
        for copy in copies:
            copy.start()
        acc[...] = jnp.zeros_like(acc)
        o_buf[...] = jnp.zeros_like(o_buf)
        for copy in copies:
            copy.wait()

    counts, offsets, tiles = row_offsets(count_ref, expert)
    x_buf[tile_span(tiles - 1), :] = jnp.zeros((TILE, x_buf.shape[1]), BF16)

    def write(src, hot, span):
        x_buf[span, :] = dot_nn(hot.astype(BF16), u_buf[src * tok:(src + 1) * tok, :]).astype(BF16)

    gather(counts, offsets, rank_ref, capacity, tok, write)

    def tile_step(tile, carry):
        rows = x_buf[tile_span(tile), :]
        for cols in f_chunks(h_buf.shape[1]):
            pre_gate = dot_nt(rows, wg_ref[0, 0, cols, :])
            pre_up = dot_nt(rows, wu_ref[0, 0, cols, :])
            act, _ = silu_parts(pre_gate)
            h_buf[:, cols] = (act * pre_up).astype(BF16)
        o_buf[tile_span(tile), :] = dot_nn(h_buf[...], wd_ref[0, 0]).astype(BF16)
        return carry

    lax.fori_loop(0, tiles, tile_step, 0)

    combine(counts, offsets, rank_t_ref, gate_t_ref, o_buf, acc, capacity, tok)

    @pl.when(expert == pl.num_programs(0) - 1)
    def _():
        put_out(acc, outs)


def input_grad_kernel(n_u, n_dy, n_out, capacity, *refs):
    count_ref, refs = refs[0], refs[1:]
    u_pieces, refs = refs[:n_u], refs[n_u:]
    dy_pieces, refs = refs[:n_dy], refs[n_dy:]
    rank_ref, gate_ref, rank_t_ref, gate_t_ref, wg_ref, wu_ref, wd_ref = refs[:7]
    outs, refs = refs[7:7 + n_out], refs[7 + n_out:]
    kept, refs = refs[:5], refs[5:]
    u_buf, dy_buf, x_buf, c_buf, v_buf, h_buf, da_buf, db_buf, acc, sems, keep_sems = refs
    expert = pl.program_id(0)
    tok = rank_t_ref.shape[1]

    @pl.when(expert == 0)
    def _():
        copies = fetch(u_pieces, u_buf, sems, 0) + fetch(dy_pieces, dy_buf, sems, n_u)
        for copy in copies:
            copy.start()
        acc[...] = jnp.zeros_like(acc)
        v_buf[...] = jnp.zeros_like(v_buf)
        for copy in copies:
            copy.wait()

    counts, offsets, tiles = row_offsets(count_ref, expert)
    x_buf[tile_span(tiles - 1), :] = jnp.zeros((TILE, x_buf.shape[1]), BF16)
    c_buf[tile_span(tiles - 1), :] = jnp.zeros((TILE, c_buf.shape[1]), BF16)

    def write(src, hot, span):
        pick = hot.astype(BF16)
        toks = slice(src * tok, (src + 1) * tok)
        gate = jnp.sum(hot * gate_ref[0, src:src + 1, :], axis=1, keepdims=True)
        x_buf[span, :] = dot_nn(pick, u_buf[toks, :]).astype(BF16)
        c_buf[span, :] = (gate * dot_nn(pick, dy_buf[toks, :])).astype(BF16)

    gather(counts, offsets, rank_ref, capacity, tok, write)

    def tile_step(tile, carry):
        span = tile_span(tile)
        keep = [pltpu.make_async_copy(src, dst.at[expert, span], keep_sems.at[i]) for i, (src, dst) in enumerate(
            zip((x_buf.at[span], c_buf.at[span], h_buf, da_buf, db_buf), kept))]
        keep[0].start()
        keep[1].start()
        rows = x_buf[span, :]
        grads = c_buf[span, :]
        for cols in f_chunks(h_buf.shape[1]):
            pre_gate = dot_nt(rows, wg_ref[0, 0, cols, :])
            pre_up = dot_nt(rows, wu_ref[0, 0, cols, :])
            d_hid = dot_nt(grads, wd_ref[0, 0, cols, :])
            act, slope = silu_parts(pre_gate)
            h_buf[:, cols] = (act * pre_up).astype(BF16)
            da_buf[:, cols] = (d_hid * pre_up * slope).astype(BF16)
            db_buf[:, cols] = (d_hid * act).astype(BF16)
        for copy in keep[2:]:
            copy.start()
        v_buf[span, :] = (dot_nn(da_buf[...], wg_ref[0, 0]) + dot_nn(db_buf[...], wu_ref[0, 0])).astype(BF16)
        for copy in keep:
            copy.wait()
        return carry

    lax.fori_loop(0, tiles, tile_step, 0)

    combine(counts, offsets, rank_t_ref, gate_t_ref, v_buf, acc, capacity, tok)

    @pl.when(expert == pl.num_programs(0) - 1)
    def _():
        put_out(acc, outs)


def weight_grad_kernel(first, count_ref, x_hbm, c_hbm, h_hbm, da_hbm, db_hbm, out_ref,
                       x_buf, c_buf, h_buf, da_buf, db_buf, acc, slot_ref, sems):
    step = pl.program_id(0)
    n_step = pl.num_programs(0)
    expert = step + first
    tiles = row_offsets(count_ref, expert)[2]

    def copies(which, tile, slot):
        return [pltpu.make_async_copy(src.at[which, tile_span(tile)], dst.at[slot], sems.at[slot, i])
                for i, (src, dst) in enumerate(((x_hbm, x_buf), (c_hbm, c_buf), (h_hbm, h_buf),
                                                (da_hbm, da_buf), (db_hbm, db_buf)))]

    @pl.when(step == 0)
    def _():
        slot_ref[0] = 0
        for copy in copies(expert, 0, 0):
            copy.start()

    def tile_step(tile, slot):
        for copy in copies(expert, tile, slot):
            copy.wait()
        after = 1 - slot

        @pl.when(tile + 1 < tiles)
        def _():
            for copy in copies(expert, tile + 1, after):
                copy.start()

        @pl.when(jnp.logical_and(tile + 1 == tiles, step + 1 < n_step))
        def _():
            for copy in copies(expert + 1, 0, after):
                copy.start()

        begin = tile == 0
        for cols in f_chunks(h_buf.shape[2]):
            acc[0, cols, :] = jnp.where(begin, 0.0, acc[0, cols, :]) + dot_tn(da_buf[slot, :, cols], x_buf[slot])
            acc[1, cols, :] = jnp.where(begin, 0.0, acc[1, cols, :]) + dot_tn(db_buf[slot, :, cols], x_buf[slot])
            acc[2, cols, :] = jnp.where(begin, 0.0, acc[2, cols, :]) + dot_tn(h_buf[slot, :, cols], c_buf[slot])
        return after

    slot_ref[0] = lax.fori_loop(0, tiles, tile_step, slot_ref[0])
    out_ref[0] = acc[...].astype(BF16)


def grad_sum_kernel(own_ref, other_ref, *refs):
    outs = refs[-3:]
    for kind, out in enumerate(outs):
        out[0, 0] = (own_ref[0, kind].astype(F32) + other_ref[0, kind].astype(F32)).astype(BF16)


ANY = pl.BlockSpec(memory_space=pl.ANY)
VMEM = pl.BlockSpec(memory_space=pltpu.VMEM)


def per_expert(shape):
    rest = (0,) * (len(shape) - 1)
    return pl.BlockSpec((1,) + tuple(shape[1:]), lambda e, *_: (e,) + rest)


def layer_weight(layer, shape):
    return pl.BlockSpec((1, 1) + tuple(shape[2:]), lambda e, *_: (layer, e, 0, 0))


def sizes(tables, weights):
    tok = tables[1].shape[2]
    capacity = tok * 3 // 4
    rows_max = (SOURCES * capacity + TILE - 1) // TILE * TILE
    _, n_local, width, d_model = weights[0].shape
    return tok, capacity, rows_max, n_local, width, d_model


def cost(n_dots, d_model, width, n_bytes):
    return pl.CostEstimate(flops=n_dots * 2 * 5 * TILE * d_model * width * 3, bytes_accessed=n_bytes, transcendentals=0)


def expert_forward(layer, u_pieces, tables, weights, out_rows):
    tok, capacity, rows_max, n_local, width, d_model = sizes(tables, weights)
    counts, rank, _, rank_t, gate_t = tables
    n_in, n_out = len(u_pieces), len(out_rows)
    return pl.pallas_call(
        functools.partial(forward_kernel, n_in, n_out, capacity),
        out_shape=[jax.ShapeDtypeStruct((rows, d_model), BF16) for rows in out_rows],
        grid_spec=pltpu.PrefetchScalarGridSpec(
            num_scalar_prefetch=1,
            grid=(n_local,),
            in_specs=[ANY] * n_in + [per_expert(t.shape) for t in (rank, rank_t, gate_t)]
            + [layer_weight(layer, w.shape) for w in weights],
            out_specs=[VMEM] * n_out,
            scratch_shapes=[pltpu.VMEM((SOURCES * tok, d_model), BF16),
                            pltpu.VMEM((rows_max + SUB, d_model), BF16),
                            pltpu.VMEM((rows_max + SUB, d_model), BF16),
                            pltpu.VMEM((TILE, width), BF16),
                            pltpu.VMEM((SOURCES * tok, d_model), F32),
                            pltpu.SemaphoreType.DMA((n_in,))]),
        compiler_params=pltpu.CompilerParams(vmem_limit_bytes=VMEM_LIMIT),
        cost_estimate=cost(3, d_model, width, 3 * 2 * n_local * d_model * width),
        name='expert_forward',
    )(counts, *u_pieces, rank, rank_t, gate_t, *weights)


def expert_input_grad(layer, u_pieces, dy_pieces, tables, weights, out_rows):
    tok, capacity, rows_max, n_local, width, d_model = sizes(tables, weights)
    counts, rank, gate, rank_t, gate_t = tables
    n_u, n_dy, n_out = len(u_pieces), len(dy_pieces), len(out_rows)
    kept = [jax.ShapeDtypeStruct((n_local, rows_max, cols), BF16) for cols in (d_model, d_model, width, width, width)]
    out = pl.pallas_call(
        functools.partial(input_grad_kernel, n_u, n_dy, n_out, capacity),
        out_shape=[jax.ShapeDtypeStruct((rows, d_model), BF16) for rows in out_rows] + kept,
        grid_spec=pltpu.PrefetchScalarGridSpec(
            num_scalar_prefetch=1,
            grid=(n_local,),
            in_specs=[ANY] * (n_u + n_dy) + [per_expert(t.shape) for t in (rank, gate, rank_t, gate_t)]
            + [layer_weight(layer, w.shape) for w in weights],
            out_specs=[VMEM] * n_out + [ANY] * 5,
            scratch_shapes=[pltpu.VMEM((SOURCES * tok, d_model), BF16)] * 2
            + [pltpu.VMEM((rows_max + SUB, d_model), BF16)] * 3
            + [pltpu.VMEM((TILE, width), BF16)] * 3
            + [pltpu.VMEM((SOURCES * tok, d_model), F32),
               pltpu.SemaphoreType.DMA((n_u + n_dy,)),
               pltpu.SemaphoreType.DMA((5,))]),
        compiler_params=pltpu.CompilerParams(vmem_limit_bytes=VMEM_LIMIT),
        cost_estimate=cost(5, d_model, width, 3 * 2 * n_local * d_model * width),
        name='expert_input_grad',
    )(counts, *u_pieces, *dy_pieces, rank, gate, rank_t, gate_t, *weights)
    return out[:n_out], out[n_out:]


def expert_weight_grad(counts, kept, first, n_expert):
    _, _, d_model = kept[0].shape
    width = kept[2].shape[2]
    return pl.pallas_call(
        functools.partial(weight_grad_kernel, first),
        out_shape=jax.ShapeDtypeStruct((n_expert, 3, width, d_model), BF16),
        grid_spec=pltpu.PrefetchScalarGridSpec(
            num_scalar_prefetch=1,
            grid=(n_expert,),
            in_specs=[ANY] * 5,
            out_specs=per_expert((n_expert, 3, width, d_model)),
            scratch_shapes=[pltpu.VMEM((2, TILE, cols), BF16) for cols in (d_model, d_model, width, width, width)]
            + [pltpu.VMEM((3, width, d_model), F32), pltpu.SMEM((1,), jnp.int32), pltpu.SemaphoreType.DMA((2, 5))]),
        compiler_params=pltpu.CompilerParams(vmem_limit_bytes=VMEM_LIMIT),
        cost_estimate=cost(3 * n_expert // 4, d_model, width, 3 * 2 * n_expert * d_model * width),
        name='expert_weight_grad',
    )(counts, *kept)


def grad_sum(layer, n_layers, n_local, first, own, other, into):
    n_expert, _, width, d_model = own.shape
    rows = width // 2
    part = pl.BlockSpec((1, 3, rows, d_model), lambda e, r: (e, 0, r, 0))
    place = pl.BlockSpec((1, 1, rows, d_model), lambda e, r: (layer, first + e, r, 0))
    into = list(into or ())
    return pl.pallas_call(
        grad_sum_kernel,
        out_shape=[jax.ShapeDtypeStruct((n_layers, n_local, width, d_model), BF16)] * 3,
        grid=(n_expert, 2),
        in_specs=[part, part] + [ANY] * len(into),
        out_specs=[place] * 3,
        input_output_aliases={2 + i: i for i in range(len(into))},
        compiler_params=pltpu.CompilerParams(vmem_limit_bytes=VMEM_LIMIT),
        cost_estimate=pl.CostEstimate(flops=n_expert * 3 * width * d_model * 256, bytes_accessed=0, transcendentals=0),
        name='grad_sum',
    )(own, other, *into)


def hop(value, axis, step):
    n = lax.axis_size(axis)
    return lax.ppermute(value, axis, [(i, i ^ step) for i in range(n)])


def spread_direct(own):
    return [own, hop(own, 'ep', 1), hop(own, 'ep', 2), hop(own, 'ep', 3)]


def spread_relay(own):
    half = own.shape[0] // 2
    low, high = own[:half], own[half:]
    x_low, y_high = hop(low, 'ep', 1), hop(high, 'ep', 2)
    x_high, y_low = hop(high, 'ep', 1), hop(low, 'ep', 2)
    return [own, x_low, x_high, y_low, y_high, hop(x_low, 'ep', 2), hop(y_high, 'ep', 1)]


def to_f32(values):
    return [value.astype(F32) for value in values]


def collect_direct(base, parts):
    own, x_part, y_part, far = parts
    terms = to_f32([base, own, hop(x_part, 'ep', 1), hop(y_part, 'ep', 2), hop(far, 'ep', 3)])
    return sum(terms[1:], terms[0]).astype(BF16)


def collect_relay(base, parts):
    own, x_low, x_high, y_low, y_high, far_low, far_high = parts
    half = x_low.shape[0]
    via_x, via_y = hop(far_low, 'ep', 1), hop(far_high, 'ep', 2)
    got_x_low, got_y_high = hop(x_low, 'ep', 1), hop(y_high, 'ep', 2)
    got_y_low = hop((y_low.astype(F32) + via_x.astype(F32)).astype(BF16), 'ep', 2)
    got_x_high = hop((x_high.astype(F32) + via_y.astype(F32)).astype(BF16), 'ep', 1)
    low = to_f32([base[:half], own[:half], got_x_low, got_y_low])
    high = to_f32([base[half:], own[half:], got_x_high, got_y_high])
    return jnp.concatenate([sum(low[1:], low[0]), sum(high[1:], high[0])], axis=0).astype(BF16)


def take(value, index, rows):
    return lax.dynamic_slice_in_dim(value, index * rows, rows, 0)


def sum_everywhere(value):
    core, chip = lax.axis_index('dp'), lax.axis_index('ep')
    half = value.shape[0] // 2
    rows = half // 4
    other = hop(take(value, 1 - core, half), 'dp', 1)
    value = (take(value, core, half).astype(F32) + other.astype(F32)).astype(BF16)
    terms = [take(value, chip, rows)] + [hop(take(value, chip ^ step, rows), 'ep', step) for step in (1, 2, 3)]
    terms = to_f32(terms)
    own = sum(terms[1:], terms[0]).astype(BF16)
    near = spread_direct(own)
    value = jnp.stack(near)[chip ^ jnp.arange(4)].reshape(half, value.shape[1])
    other = hop(value, 'dp', 1)
    return jnp.where(core == 0, jnp.concatenate([value, other]), jnp.concatenate([other, value]))


def route_tables(expert_ids, gate_vals, n_local):
    packed = jnp.concatenate([expert_ids.astype(F32), gate_vals], axis=2)
    packed = jnp.stack(spread_direct(packed))
    top_k = expert_ids.shape[2]
    tok = expert_ids.shape[1]
    ids = packed[..., :top_k].astype(jnp.int32)
    gates = packed[..., top_k:]
    mine = lax.axis_index('ep') * n_local + jnp.arange(n_local)
    hits = ids[:, :, None] == mine[None, None, :, None, None]
    chosen = jnp.any(hits, axis=-1)
    gate = jnp.sum(jnp.where(hits, gates[:, :, None], 0.0), axis=-1)
    upto = (jnp.arange(tok)[:, None] <= jnp.arange(tok)[None, :]).astype(BF16)
    order = jnp.einsum('slet,tv->slev', chosen.astype(BF16), upto, preferred_element_type=F32)
    counts = order[..., -1].astype(jnp.int32)
    rank = jnp.where(chosen, order.astype(jnp.int32) - 1, -1)
    return [(counts[:, layer].T, rank[:, layer].transpose(1, 0, 2), gate[:, layer].transpose(1, 0, 2),
             rank[:, layer].transpose(1, 2, 0), gate[:, layer].transpose(1, 2, 0))
            for layer in range(expert_ids.shape[0])]


def after(value, *others):
    return lax.optimization_barrier((value, others))[0]


def mix_in(x_in, w_mix):
    return (x_in.astype(F32) + jnp.dot(x_in, w_mix, preferred_element_type=F32)).astype(BF16)


def mix_back(d_u, w_mix):
    return (d_u.astype(F32) + jnp.einsum('te,de->td', d_u, w_mix, preferred_element_type=F32)).astype(BF16)


def mix_grad(x_in, d_u):
    return jnp.einsum('td,te->de', x_in, d_u, preferred_element_type=F32).astype(BF16)


def solution(mesh):
    tok_spec = P(('dp', 'ep'), None)
    route_spec = P(None, ('dp', 'ep'), None)
    whole_spec = P(None, None, None)
    expert_spec = P(None, 'ep', None, None)

    def device_body(tokens, d_out, expert_ids, gate_vals, w_mix, w_gate, w_up, w_down):
        n_layers = w_mix.shape[0]
        n_local = w_gate.shape[1]
        last = n_layers - 1
        tok = tokens.shape[0]
        whole = [tok] * SOURCES
        halves = [tok] + [tok // 2] * (2 * SOURCES - 2)
        weights = (jnp.swapaxes(w_gate, 2, 3), jnp.swapaxes(w_up, 2, 3), w_down)

        x_in = [tokens]
        u_all = [spread_relay(mix_in(tokens, w_mix[0]))]
        tables = route_tables(expert_ids, gate_vals, n_local)
        for layer in range(last):
            parts = expert_forward(layer, u_all[layer], tables[layer], weights, halves)
            if layer == 0:
                dy_all = spread_direct(after(d_out, u_all[0]))
            x_in.append(collect_relay(u_all[layer][0], parts))
            u_all.append(spread_relay(mix_in(x_in[-1], w_mix[layer + 1])))

        d_y, grads, mixes, left = d_out, None, [None] * n_layers, []
        for layer in reversed(range(n_layers)):
            counts = tables[layer][0]
            parts, kept = expert_input_grad(layer, u_all[layer], dy_all, tables[layer], weights, whole)
            if layer == last:
                top = expert_forward(layer, after(u_all[layer], parts[0]), tables[layer], weights, whole)
                kept = after(kept, top)
            half = n_local // 2
            for first in (0, half):
                own = expert_weight_grad(counts, kept, first, half)
                left.append((layer, first, own, hop(own, 'dp', 1)))
            d_u = collect_direct(d_y, parts)
            mixes[layer] = sum_everywhere(mix_grad(x_in[layer], d_u))
            d_y = mix_back(d_u, w_mix[layer])
            if layer > 0:
                near = spread_direct(d_y)
                dy_all = after(near, left[-1][2])
            if layer == last:
                layer_out = collect_direct(u_all[last][0], after(top, near[1]))
        for layer, first, own, other in left:
            grads = grad_sum(layer, n_layers, n_local, first, own, other, grads)
        return (layer_out, d_y, jnp.stack(mixes), jnp.swapaxes(grads[0], 2, 3), jnp.swapaxes(grads[1], 2, 3), grads[2])

    return jax.shard_map(device_body, mesh=mesh,
                         in_specs=(tok_spec, tok_spec, route_spec, route_spec, whole_spec,
                                   expert_spec, expert_spec, expert_spec),
                         out_specs=(tok_spec, tok_spec, whole_spec, expert_spec, expert_spec, expert_spec),
                         check_vma=False)
```

```python
import functools

import jax
import jax.numpy as jnp
from jax import lax
from jax.experimental import pallas as pl
from jax.experimental.pallas import tpu as pltpu
from jax.sharding import PartitionSpec as P


TILE = 384
SUB = 128
ALIGN = 16
F_CHUNK = 512
SOURCES = 4
VMEM_LIMIT = 62 * 1024 * 1024
BF16 = jnp.bfloat16
F32 = jnp.float32


def silu_parts(pre_gate):
    sig_val = jax.nn.sigmoid(pre_gate)
    return pre_gate * sig_val, sig_val * (1.0 + pre_gate * (1.0 - sig_val))


def dot_nn(lhs, rhs):
    return lax.dot_general(lhs, rhs, (((1,), (0,)), ((), ())), preferred_element_type=F32)


def dot_nt(lhs, rhs):
    return lax.dot_general(lhs, rhs, (((1,), (1,)), ((), ())), preferred_element_type=F32)


def dot_tn(lhs, rhs):
    return lax.dot_general(lhs, rhs, (((0,), (0,)), ((), ())), preferred_element_type=F32)


def f_chunks(width):
    return [slice(lo, min(lo + F_CHUNK, width)) for lo in range(0, width, F_CHUNK)]


def tile_span(tile):
    return pl.ds(pl.multiple_of(tile * TILE, TILE), TILE)


def row_offsets(count_ref, expert):
    counts = [count_ref[expert, src] for src in range(SOURCES)]
    offsets = [jnp.int32(0)]
    for count in counts:
        offsets.append(offsets[-1] + (count + ALIGN - 1) // ALIGN * ALIGN)
    total = offsets.pop()
    return counts, offsets, jnp.maximum((total + TILE - 1) // TILE, 1)


def per_source(counts, run, capacity):
    small = functools.reduce(jnp.maximum, counts) <= SUB

    @pl.when(small)
    def _():
        for src in range(SOURCES):
            run(src, SUB)

    @pl.when(jnp.logical_not(small))
    def _():
        for src in range(SOURCES):
            pl.when(counts[src] <= SUB)(functools.partial(run, src, SUB))
            pl.when(counts[src] > SUB)(functools.partial(run, src, capacity))


def fetch(pieces, buf, sems, base):
    copies, row = [], 0
    for index, piece in enumerate(pieces):
        rows = piece.shape[0]
        copies.append(pltpu.make_async_copy(piece, buf.at[pl.ds(row, rows)], sems.at[base + index]))
        row += rows
    return copies


def gather(counts, offsets, rank_ref, capacity, tok, write):
    def run(src, rows):
        want = lax.broadcasted_iota(jnp.int32, (rows, tok), 0)
        hot = (rank_ref[0, src:src + 1, :] == want).astype(F32)
        write(src, hot, pl.ds(pl.multiple_of(offsets[src], ALIGN), rows))

    per_source(counts, run, capacity)


def combine(counts, offsets, rank_t_ref, gate_t_ref, buf, acc, capacity, tok):
    def run(src, rows):
        want = lax.broadcasted_iota(jnp.int32, (tok, rows), 1)
        pick = (rank_t_ref[0, :, src:src + 1] == want).astype(BF16)
        values = buf[pl.ds(pl.multiple_of(offsets[src], ALIGN), rows), :]
        span = slice(src * tok, (src + 1) * tok)
        acc[span, :] += gate_t_ref[0, :, src:src + 1] * dot_nn(pick, values)

    per_source(counts, run, capacity)


def put_out(acc, out_refs):
    row = 0
    for out in out_refs:
        rows = out.shape[0]
        out[...] = acc[row:row + rows, :].astype(BF16)
        row += rows


def forward_kernel(n_in, n_out, capacity, *refs):
    count_ref, refs = refs[0], refs[1:]
    u_pieces, refs = refs[:n_in], refs[n_in:]
    rank_ref, rank_t_ref, gate_t_ref, wg_ref, wu_ref, wd_ref = refs[:6]
    outs, refs = refs[6:6 + n_out], refs[6 + n_out:]
    u_buf, x_buf, o_buf, h_buf, acc, sems = refs
    expert = pl.program_id(0)
    tok = rank_t_ref.shape[1]

    @pl.when(expert == 0)
    def _():
        copies = fetch(u_pieces, u_buf, sems, 0)
        for copy in copies:
            copy.start()
        acc[...] = jnp.zeros_like(acc)
        o_buf[...] = jnp.zeros_like(o_buf)
        for copy in copies:
            copy.wait()

    counts, offsets, tiles = row_offsets(count_ref, expert)
    x_buf[tile_span(tiles - 1), :] = jnp.zeros((TILE, x_buf.shape[1]), BF16)

    def write(src, hot, span):
        x_buf[span, :] = dot_nn(hot.astype(BF16), u_buf[src * tok:(src + 1) * tok, :]).astype(BF16)

    gather(counts, offsets, rank_ref, capacity, tok, write)

    def tile_step(tile, carry):
        rows = x_buf[tile_span(tile), :]
        for cols in f_chunks(h_buf.shape[1]):
            pre_gate = dot_nt(rows, wg_ref[0, 0, cols, :])
            pre_up = dot_nt(rows, wu_ref[0, 0, cols, :])
            act, _ = silu_parts(pre_gate)
            h_buf[:, cols] = (act * pre_up).astype(BF16)
        o_buf[tile_span(tile), :] = dot_nn(h_buf[...], wd_ref[0, 0]).astype(BF16)
        return carry

    lax.fori_loop(0, tiles, tile_step, 0)

    combine(counts, offsets, rank_t_ref, gate_t_ref, o_buf, acc, capacity, tok)

    @pl.when(expert == pl.num_programs(0) - 1)
    def _():
        put_out(acc, outs)


def input_grad_kernel(n_u, n_dy, n_out, capacity, forward, *refs):
    count_ref, refs = refs[0], refs[1:]
    u_pieces, refs = refs[:n_u], refs[n_u:]
    dy_pieces, refs = refs[:n_dy], refs[n_dy:]
    rank_ref, gate_ref, rank_t_ref, gate_t_ref, wg_ref, wu_ref, wd_ref = refs[:7]
    refs = refs[7:]
    outs, refs = refs[:n_out], refs[n_out:]
    tops, refs = (refs[:n_out], refs[n_out:]) if forward else ((), refs)
    kept, refs = refs[:5], refs[5:]
    u_buf, dy_buf, x_buf, c_buf, v_buf, h_buf, da_buf, db_buf, acc, slot_ref, sems, keep_sems = refs[:12]
    expert = pl.program_id(0)
    last = expert == pl.num_programs(0) - 1
    tok = rank_t_ref.shape[1]
    if forward:
        o_buf, top_acc = refs[12:]

    def keep_cols(tile, slot):
        return [pltpu.make_async_copy(src.at[slot], dst.at[expert, tile_span(tile)], keep_sems.at[slot, i])
                for i, (src, dst) in enumerate(((h_buf, kept[2]), (da_buf, kept[3]), (db_buf, kept[4])))]

    def keep_rows(tile):
        span = tile_span(tile)
        return [pltpu.make_async_copy(src.at[span], dst.at[expert, span], keep_sems.at[2, i])
                for i, (src, dst) in enumerate(((x_buf, kept[0]), (c_buf, kept[1])))]

    @pl.when(expert == 0)
    def _():
        copies = fetch(u_pieces, u_buf, sems, 0) + fetch(dy_pieces, dy_buf, sems, n_u)
        for copy in copies:
            copy.start()
        slot_ref[0] = 0
        acc[...] = jnp.zeros_like(acc)
        v_buf[...] = jnp.zeros_like(v_buf)
        if forward:
            top_acc[...] = jnp.zeros_like(top_acc)
            o_buf[...] = jnp.zeros_like(o_buf)
        for copy in copies:
            copy.wait()

    counts, offsets, tiles = row_offsets(count_ref, expert)
    x_buf[tile_span(tiles - 1), :] = jnp.zeros((TILE, x_buf.shape[1]), BF16)
    c_buf[tile_span(tiles - 1), :] = jnp.zeros((TILE, c_buf.shape[1]), BF16)

    def write(src, hot, span):
        pick = hot.astype(BF16)
        toks = slice(src * tok, (src + 1) * tok)
        gate = jnp.sum(hot * gate_ref[0, src:src + 1, :], axis=1, keepdims=True)
        x_buf[span, :] = dot_nn(pick, u_buf[toks, :]).astype(BF16)
        c_buf[span, :] = (gate * dot_nn(pick, dy_buf[toks, :])).astype(BF16)

    gather(counts, offsets, rank_ref, capacity, tok, write)

    def tile_step(tile, slot):
        span = tile_span(tile)
        rows_out = keep_rows(tile)
        for copy in rows_out:
            copy.start()
        rows = x_buf[span, :]
        grads = c_buf[span, :]
        for cols in f_chunks(h_buf.shape[2]):
            pre_gate = dot_nt(rows, wg_ref[0, 0, cols, :])
            pre_up = dot_nt(rows, wu_ref[0, 0, cols, :])
            d_hid = dot_nt(grads, wd_ref[0, 0, cols, :])
            act, slope = silu_parts(pre_gate)
            h_buf[slot, :, cols] = (act * pre_up).astype(BF16)
            da_buf[slot, :, cols] = (d_hid * pre_up * slope).astype(BF16)
            db_buf[slot, :, cols] = (d_hid * act).astype(BF16)
        cols_out = keep_cols(tile, slot)
        for copy in cols_out:
            copy.start()
        if forward:
            o_buf[span, :] = dot_nn(h_buf[slot], wd_ref[0, 0]).astype(BF16)
        v_buf[span, :] = (dot_nn(da_buf[slot], wg_ref[0, 0]) + dot_nn(db_buf[slot], wu_ref[0, 0])).astype(BF16)
        for copy in rows_out:
            copy.wait()

        @pl.when(tile > 0)
        def _():
            for copy in keep_cols(tile - 1, 1 - slot):
                copy.wait()

        return 1 - slot

    slot = lax.fori_loop(0, tiles, tile_step, slot_ref[0])
    slot_ref[0] = slot

    combine(counts, offsets, rank_t_ref, gate_t_ref, v_buf, acc, capacity, tok)
    if forward:
        combine(counts, offsets, rank_t_ref, gate_t_ref, o_buf, top_acc, capacity, tok)
    for copy in keep_cols(tiles - 1, 1 - slot):
        copy.wait()

    @pl.when(last)
    def _():
        put_out(acc, outs)
        if forward:
            put_out(top_acc, tops)


def weight_grad_kernel(first, count_ref, x_hbm, c_hbm, h_hbm, da_hbm, db_hbm, out_ref,
                       x_buf, c_buf, h_buf, da_buf, db_buf, acc, slot_ref, sems):
    step = pl.program_id(0)
    n_step = pl.num_programs(0)
    expert = step + first
    tiles = row_offsets(count_ref, expert)[2]

    def copies(which, tile, slot):
        return [pltpu.make_async_copy(src.at[which, tile_span(tile)], dst.at[slot], sems.at[slot, i])
                for i, (src, dst) in enumerate(((x_hbm, x_buf), (c_hbm, c_buf), (h_hbm, h_buf),
                                                (da_hbm, da_buf), (db_hbm, db_buf)))]

    @pl.when(step == 0)
    def _():
        slot_ref[0] = 0
        for copy in copies(expert, 0, 0):
            copy.start()

    def tile_step(tile, slot):
        for copy in copies(expert, tile, slot):
            copy.wait()
        after = 1 - slot

        @pl.when(tile + 1 < tiles)
        def _():
            for copy in copies(expert, tile + 1, after):
                copy.start()

        @pl.when(jnp.logical_and(tile + 1 == tiles, step + 1 < n_step))
        def _():
            for copy in copies(expert + 1, 0, after):
                copy.start()

        begin = tile == 0
        for cols in f_chunks(h_buf.shape[2]):
            acc[0, cols, :] = jnp.where(begin, 0.0, acc[0, cols, :]) + dot_tn(da_buf[slot, :, cols], x_buf[slot])
            acc[1, cols, :] = jnp.where(begin, 0.0, acc[1, cols, :]) + dot_tn(db_buf[slot, :, cols], x_buf[slot])
            acc[2, cols, :] = jnp.where(begin, 0.0, acc[2, cols, :]) + dot_tn(h_buf[slot, :, cols], c_buf[slot])
        return after

    slot_ref[0] = lax.fori_loop(0, tiles, tile_step, slot_ref[0])
    out_ref[0] = acc[...].astype(BF16)


def grad_sum_kernel(own_ref, other_ref, *refs):
    outs = refs[-3:]
    for kind, out in enumerate(outs):
        out[0, 0] = (own_ref[0, kind].astype(F32) + other_ref[0, kind].astype(F32)).astype(BF16)


ANY = pl.BlockSpec(memory_space=pl.ANY)
VMEM = pl.BlockSpec(memory_space=pltpu.VMEM)


def per_expert(shape):
    rest = (0,) * (len(shape) - 1)
    return pl.BlockSpec((1,) + tuple(shape[1:]), lambda e, *_: (e,) + rest)


def layer_weight(layer, shape):
    return pl.BlockSpec((1, 1) + tuple(shape[2:]), lambda e, *_: (layer, e, 0, 0))


def sizes(tables, weights):
    tok = tables[1].shape[2]
    capacity = tok * 3 // 4
    rows_max = (SOURCES * capacity + TILE - 1) // TILE * TILE
    _, n_local, width, d_model = weights[0].shape
    return tok, capacity, rows_max, n_local, width, d_model


def cost(n_dots, d_model, width, n_bytes):
    return pl.CostEstimate(flops=n_dots * 2 * 5 * TILE * d_model * width * 3, bytes_accessed=n_bytes, transcendentals=0)


def expert_forward(layer, u_pieces, tables, weights, out_rows):
    tok, capacity, rows_max, n_local, width, d_model = sizes(tables, weights)
    counts, rank, _, rank_t, gate_t = tables
    n_in, n_out = len(u_pieces), len(out_rows)
    return pl.pallas_call(
        functools.partial(forward_kernel, n_in, n_out, capacity),
        out_shape=[jax.ShapeDtypeStruct((rows, d_model), BF16) for rows in out_rows],
        grid_spec=pltpu.PrefetchScalarGridSpec(
            num_scalar_prefetch=1,
            grid=(n_local,),
            in_specs=[ANY] * n_in + [per_expert(t.shape) for t in (rank, rank_t, gate_t)]
            + [layer_weight(layer, w.shape) for w in weights],
            out_specs=[VMEM] * n_out,
            scratch_shapes=[pltpu.VMEM((SOURCES * tok, d_model), BF16),
                            pltpu.VMEM((rows_max + SUB, d_model), BF16),
                            pltpu.VMEM((rows_max + SUB, d_model), BF16),
                            pltpu.VMEM((TILE, width), BF16),
                            pltpu.VMEM((SOURCES * tok, d_model), F32),
                            pltpu.SemaphoreType.DMA((n_in,))]),
        compiler_params=pltpu.CompilerParams(vmem_limit_bytes=VMEM_LIMIT),
        cost_estimate=cost(3, d_model, width, 3 * 2 * n_local * d_model * width),
        name='expert_forward',
    )(counts, *u_pieces, rank, rank_t, gate_t, *weights)


def expert_input_grad(layer, u_pieces, dy_pieces, tables, weights, out_rows, forward):
    tok, capacity, rows_max, n_local, width, d_model = sizes(tables, weights)
    counts, rank, gate, rank_t, gate_t = tables
    n_u, n_dy, n_out = len(u_pieces), len(dy_pieces), len(out_rows)
    kept = [jax.ShapeDtypeStruct((n_local, rows_max, cols), BF16) for cols in (d_model, d_model, width, width, width)]
    sums = [jax.ShapeDtypeStruct((rows, d_model), BF16) for rows in out_rows] * (1 + forward)
    row_buf = pltpu.VMEM((rows_max + SUB, d_model), BF16)
    token_acc = pltpu.VMEM((SOURCES * tok, d_model), F32)
    out = pl.pallas_call(
        functools.partial(input_grad_kernel, n_u, n_dy, n_out, capacity, forward),
        out_shape=sums + kept,
        grid_spec=pltpu.PrefetchScalarGridSpec(
            num_scalar_prefetch=1,
            grid=(n_local,),
            in_specs=[ANY] * (n_u + n_dy) + [per_expert(t.shape) for t in (rank, gate, rank_t, gate_t)]
            + [layer_weight(layer, w.shape) for w in weights],
            out_specs=[VMEM] * len(sums) + [ANY] * 5,
            scratch_shapes=[pltpu.VMEM((SOURCES * tok, d_model), BF16)] * 2 + [row_buf] * 3
            + [pltpu.VMEM((2, TILE, width), BF16)] * 3
            + [token_acc, pltpu.SMEM((1,), jnp.int32),
               pltpu.SemaphoreType.DMA((n_u + n_dy,)),
               pltpu.SemaphoreType.DMA((3, 3))]
            + [row_buf, token_acc] * forward),
        compiler_params=pltpu.CompilerParams(vmem_limit_bytes=VMEM_LIMIT),
        cost_estimate=cost(5 + forward, d_model, width, 3 * 2 * n_local * d_model * width),
        name='expert_input_grad',
    )(counts, *u_pieces, *dy_pieces, rank, gate, rank_t, gate_t, *weights)
    return out[:n_out], out[n_out:len(sums)], out[len(sums):]


def expert_weight_grad(counts, kept, first, n_expert):
    _, _, d_model = kept[0].shape
    width = kept[2].shape[2]
    return pl.pallas_call(
        functools.partial(weight_grad_kernel, first),
        out_shape=jax.ShapeDtypeStruct((n_expert, 3, width, d_model), BF16),
        grid_spec=pltpu.PrefetchScalarGridSpec(
            num_scalar_prefetch=1,
            grid=(n_expert,),
            in_specs=[ANY] * 5,
            out_specs=per_expert((n_expert, 3, width, d_model)),
            scratch_shapes=[pltpu.VMEM((2, TILE, cols), BF16) for cols in (d_model, d_model, width, width, width)]
            + [pltpu.VMEM((3, width, d_model), F32), pltpu.SMEM((1,), jnp.int32), pltpu.SemaphoreType.DMA((2, 5))]),
        compiler_params=pltpu.CompilerParams(vmem_limit_bytes=VMEM_LIMIT),
        cost_estimate=cost(3 * n_expert // 4, d_model, width, 3 * 2 * n_expert * d_model * width),
        name='expert_weight_grad',
    )(counts, *kept)


def grad_sum(layer, n_layers, n_local, first, own, other, into):
    n_expert, _, width, d_model = own.shape
    rows = width // 2
    part = pl.BlockSpec((1, 3, rows, d_model), lambda e, r: (e, 0, r, 0))
    place = pl.BlockSpec((1, 1, rows, d_model), lambda e, r: (layer, first + e, r, 0))
    into = list(into or ())
    return pl.pallas_call(
        grad_sum_kernel,
        out_shape=[jax.ShapeDtypeStruct((n_layers, n_local, width, d_model), BF16)] * 3,
        grid=(n_expert, 2),
        in_specs=[part, part] + [ANY] * len(into),
        out_specs=[place] * 3,
        input_output_aliases={2 + i: i for i in range(len(into))},
        compiler_params=pltpu.CompilerParams(vmem_limit_bytes=VMEM_LIMIT),
        cost_estimate=pl.CostEstimate(flops=n_expert * 3 * width * d_model * 256, bytes_accessed=0, transcendentals=0),
        name='grad_sum',
    )(own, other, *into)


def hop(value, axis, step):
    n = lax.axis_size(axis)
    return lax.ppermute(value, axis, [(i, i ^ step) for i in range(n)])


def spread_direct(own):
    return [own, hop(own, 'ep', 1), hop(own, 'ep', 2), hop(own, 'ep', 3)]


def spread_relay(own):
    half = own.shape[0] // 2
    low, high = own[:half], own[half:]
    x_low, y_high = hop(low, 'ep', 1), hop(high, 'ep', 2)
    x_high, y_low = hop(high, 'ep', 1), hop(low, 'ep', 2)
    return [own, x_low, x_high, y_low, y_high, hop(x_low, 'ep', 2), hop(y_high, 'ep', 1)]


def to_f32(values):
    return [value.astype(F32) for value in values]


def collect_direct(base, parts):
    own, x_part, y_part, far = parts
    terms = to_f32([base, own, hop(x_part, 'ep', 1), hop(y_part, 'ep', 2), hop(far, 'ep', 3)])
    return sum(terms[1:], terms[0]).astype(BF16)


def collect_relay(base, parts):
    own, x_low, x_high, y_low, y_high, far_low, far_high = parts
    half = x_low.shape[0]
    via_x, via_y = hop(far_low, 'ep', 1), hop(far_high, 'ep', 2)
    got_x_low, got_y_high = hop(x_low, 'ep', 1), hop(y_high, 'ep', 2)
    got_y_low = hop((y_low.astype(F32) + via_x.astype(F32)).astype(BF16), 'ep', 2)
    got_x_high = hop((x_high.astype(F32) + via_y.astype(F32)).astype(BF16), 'ep', 1)
    low = to_f32([base[:half], own[:half], got_x_low, got_y_low])
    high = to_f32([base[half:], own[half:], got_x_high, got_y_high])
    return jnp.concatenate([sum(low[1:], low[0]), sum(high[1:], high[0])], axis=0).astype(BF16)


def take(value, index, rows):
    return lax.dynamic_slice_in_dim(value, index * rows, rows, 0)


def sum_everywhere(value):
    core, chip = lax.axis_index('dp'), lax.axis_index('ep')
    half = value.shape[0] // 2
    rows = half // 4
    other = hop(take(value, 1 - core, half), 'dp', 1)
    value = (take(value, core, half).astype(F32) + other.astype(F32)).astype(BF16)
    terms = [take(value, chip, rows)] + [hop(take(value, chip ^ step, rows), 'ep', step) for step in (1, 2, 3)]
    terms = to_f32(terms)
    own = sum(terms[1:], terms[0]).astype(BF16)
    near = spread_direct(own)
    value = jnp.stack(near)[chip ^ jnp.arange(4)].reshape(half, value.shape[1])
    other = hop(value, 'dp', 1)
    return jnp.where(core == 0, jnp.concatenate([value, other]), jnp.concatenate([other, value]))


def route_tables(expert_ids, gate_vals, n_local):
    packed = jnp.concatenate([expert_ids.astype(F32), gate_vals], axis=2)
    packed = jnp.stack(spread_direct(packed))
    top_k = expert_ids.shape[2]
    tok = expert_ids.shape[1]
    ids = packed[..., :top_k].astype(jnp.int32)
    gates = packed[..., top_k:]
    mine = lax.axis_index('ep') * n_local + jnp.arange(n_local)
    hits = ids[:, :, None] == mine[None, None, :, None, None]
    chosen = jnp.any(hits, axis=-1)
    gate = jnp.sum(jnp.where(hits, gates[:, :, None], 0.0), axis=-1)
    upto = (jnp.arange(tok)[:, None] <= jnp.arange(tok)[None, :]).astype(BF16)
    order = jnp.einsum('slet,tv->slev', chosen.astype(BF16), upto, preferred_element_type=F32)
    counts = order[..., -1].astype(jnp.int32)
    rank = jnp.where(chosen, order.astype(jnp.int32) - 1, -1)
    return [(counts[:, layer].T, rank[:, layer].transpose(1, 0, 2), gate[:, layer].transpose(1, 0, 2),
             rank[:, layer].transpose(1, 2, 0), gate[:, layer].transpose(1, 2, 0))
            for layer in range(expert_ids.shape[0])]


def after(value, *others):
    return lax.optimization_barrier((value, others))[0]


def mix_in(x_in, w_mix):
    return (x_in.astype(F32) + jnp.dot(x_in, w_mix, preferred_element_type=F32)).astype(BF16)


def mix_back(d_u, w_mix):
    return (d_u.astype(F32) + jnp.einsum('te,de->td', d_u, w_mix, preferred_element_type=F32)).astype(BF16)


def mix_grad(x_in, d_u):
    return jnp.einsum('td,te->de', x_in, d_u, preferred_element_type=F32).astype(BF16)


def solution(mesh):
    tok_spec = P(('dp', 'ep'), None)
    route_spec = P(None, ('dp', 'ep'), None)
    whole_spec = P(None, None, None)
    expert_spec = P(None, 'ep', None, None)

    def device_body(tokens, d_out, expert_ids, gate_vals, w_mix, w_gate, w_up, w_down):
        n_layers = w_mix.shape[0]
        n_local = w_gate.shape[1]
        last = n_layers - 1
        tok = tokens.shape[0]
        whole = [tok] * SOURCES
        halves = [tok] + [tok // 2] * (2 * SOURCES - 2)
        weights = (jnp.swapaxes(w_gate, 2, 3), jnp.swapaxes(w_up, 2, 3), w_down)

        x_in = [tokens]
        u_all = [spread_relay(mix_in(tokens, w_mix[0]))]
        tables = route_tables(expert_ids, gate_vals, n_local)
        for layer in range(last):
            parts = expert_forward(layer, u_all[layer], tables[layer], weights, halves)
            if layer == 0:
                dy_all = spread_direct(after(d_out, u_all[0]))
            x_in.append(collect_relay(u_all[layer][0], parts))
            u_all.append(spread_relay(mix_in(x_in[-1], w_mix[layer + 1])))

        d_y, grads, mixes = d_out, None, [None] * n_layers
        for layer in reversed(range(n_layers)):
            counts = tables[layer][0]
            parts, top, kept = expert_input_grad(layer, u_all[layer], dy_all, tables[layer], weights, whole,
                                                 layer == last)
            half = n_local // 2
            left = []
            for first in (0, half):
                own = expert_weight_grad(counts, kept, first, half)
                left.append((first, own, hop(own, 'dp', 1)))
            d_u = collect_direct(d_y, parts)
            mixes[layer] = sum_everywhere(mix_grad(x_in[layer], d_u))
            d_y = mix_back(d_u, w_mix[layer])
            if layer > 0:
                dy_all = spread_direct(d_y)
            for first, own, other in left:
                grads = grad_sum(layer, n_layers, n_local, first, own, other, grads)
            if layer > 0:
                dy_all = after(dy_all, grads)
            if layer == last:
                layer_out = collect_direct(u_all[last][0], after(top, dy_all[1]))
        return (layer_out, d_y, jnp.stack(mixes), jnp.swapaxes(grads[0], 2, 3), jnp.swapaxes(grads[1], 2, 3), grads[2])

    return jax.shard_map(device_body, mesh=mesh,
                         in_specs=(tok_spec, tok_spec, route_spec, route_spec, whole_spec,
                                   expert_spec, expert_spec, expert_spec),
                         out_specs=(tok_spec, tok_spec, whole_spec, expert_spec, expert_spec, expert_spec),
                         check_vma=False)
```
